64 devices in a mesh: layer: 4 (over x, y), tensor: 16 (over z, core).
Axes of the slice: x: 2, y: 2, z: 8, core: 2. Of those that a mesh axis runs over, the one named last changes fastest.
The devices are a block of a 4x4x8 slice.
Arguments:
- gradient: bfloat16 [2048, 6144], P('layer', 'tensor'), parts along dimension 0
- left_stat: float32 [2048, 512], P(('layer', 'tensor')), parts along dimension 0
- right_stat: float32 [24576, 6144], P(('layer', 'tensor')), parts along dimension 0
- left_root: bfloat16 [2048, 512], P(('layer', 'tensor')), parts along dimension 0
- right_root: bfloat16 [24576, 6144], P(('layer', 'tensor')), parts along dimension 0
Outputs:
- output 1: float32 [2048, 512], P(('layer', 'tensor')), parts along dimension 0
- output 2: float32 [24576, 6144], P(('layer', 'tensor')), parts along dimension 0
- output 3: float32 [2048, 6144], P('layer', 'tensor'), parts along dimension 0
There are 4 independent parts. The reference program is written for one: setup_inputs(seed, part) draws one part's arguments, and reference() takes and returns one part's arrays. A program takes and returns all parts, laid end to end along the dimension named above; each array names one.
All inputs are finite; a program needn't handle non-finite values.
Results may differ from the reference program's by a relative error of at most 0.001.
Values are sent between devices in bfloat16 or wider.
A program may use at most 768 MiB of HBM per device.

```python
import jax
import jax.numpy as jnp

ROW_COUNT = 512
COL_COUNT = 6144
EMA_DECAY = 0.9


def setup_inputs(seed: int = 0, part: int = 0) -> dict:
    base_key = jax.random.fold_in(jax.random.key(seed), part)
    keys = jax.random.split(base_key, 5)
    grad_scale = (ROW_COUNT * COL_COUNT) ** -0.25
    root_scale = (ROW_COUNT * COL_COUNT) ** 0.125
    gradient = grad_scale * jax.random.normal(keys[0], (ROW_COUNT, COL_COUNT), jnp.float32)
    left_hist = jax.random.normal(keys[1], (ROW_COUNT, COL_COUNT // 8), jnp.float32)
    left_stat = (0.8 * grad_scale ** 2) * jnp.dot(left_hist, left_hist.T)
    right_hist = jax.random.normal(keys[2], (COL_COUNT, ROW_COUNT // 8), jnp.float32)
    right_stat = (0.8 * grad_scale ** 2) * jnp.dot(right_hist, right_hist.T)
    left_basis = jax.random.normal(keys[3], (ROW_COUNT, ROW_COUNT // 8), jnp.float32)
    left_root = root_scale * (0.5 * jnp.eye(ROW_COUNT, dtype=jnp.float32) + jnp.dot(left_basis, left_basis.T) / ROW_COUNT)
    right_basis = jax.random.normal(keys[4], (COL_COUNT, COL_COUNT // 8), jnp.float32)
    right_prod = jnp.dot(right_basis, right_basis.T) / COL_COUNT
    right_root = root_scale * (0.5 * jnp.eye(COL_COUNT, dtype=jnp.float32) + 0.5 * (right_prod + right_prod.T))
    return {"gradient": gradient.astype(jnp.bfloat16), "left_stat": left_stat, "right_stat": right_stat, "left_root": left_root.astype(jnp.bfloat16), "right_root": right_root.astype(jnp.bfloat16)}


def reference(gradient, left_stat, right_stat, left_root, right_root):
    left_new = EMA_DECAY * left_stat + (1.0 - EMA_DECAY) * jnp.dot(gradient, gradient.T, preferred_element_type=jnp.float32)
    right_new = EMA_DECAY * right_stat + (1.0 - EMA_DECAY) * jnp.dot(gradient.T, gradient, preferred_element_type=jnp.float32)
    precond = jnp.dot(gradient, right_root, preferred_element_type=jnp.float32).astype(jnp.bfloat16)
    direction = jnp.dot(left_root, precond, preferred_element_type=jnp.float32)
    return (left_new, right_new, direction)
```

```python
import functools

import jax
import jax.numpy as jnp
from jax import lax
from jax.experimental import pallas as pl
from jax.experimental.pallas import tpu as pltpu
from jax.sharding import PartitionSpec as P

EMA_DECAY = 0.9
CHUNKS = 4
LOADS = 4
NT = (((1,), (1,)), ((), ()))


def _dot(a, b):
    return jnp.dot(a, b, preferred_element_type=jnp.float32)


def _dot_nt(a, b):
    return lax.dot_general(a, b, NT, preferred_element_type=jnp.float32)


def _gather_kernel(
    chips,
    g_hbm, lr_hbm, l_hbm, r_hbm, rr_hbm,
    gall, lrall, rnew, rrv, xacc, lacc, lold, gt,
    load_sem, ring_send, ring_recv, sis_send, sis_recv,
    lring_send, lring_recv, lsis_send, lsis_recv,
):
    half = chips // 2
    full = half - 1
    me = lax.axis_index("tensor")
    z, core = me // 2, me % 2
    sister = {"tensor": 2 * z + (1 - core)}
    right = {"tensor": 2 * ((z + 1) % chips) + core}
    left = {"tensor": 2 * ((z + chips - 1) % chips) + core}
    towards = (right, left)
    block_rows, block_cols = g_hbm.shape
    lr_rows = lr_hbm.shape[0]
    piece = block_rows // CHUNKS
    n_full = full * CHUNKS
    n_events = n_full + CHUNKS // 2

    def chip_at(side, dist):
        return (z + chips - dist) % chips if side == 0 else (z + dist) % chips

    def piece_at(side, n):
        k = n % CHUNKS if side == 0 else (n + CHUNKS // 2) % CHUNKS
        slot = 2 * chip_at(side, n // CHUNKS) + core
        return gall.at[slot, pl.ds(pl.multiple_of(k * piece, piece), piece), :]

    def ring_copy(side, n):
        ref = piece_at(side, n)
        return pltpu.make_async_remote_copy(
            ref, ref, ring_send.at[side, n], ring_recv.at[side, n],
            device_id=towards[side], device_id_type=pl.DeviceIdType.MESH)

    def ring_arrival(side, e):
        ref = piece_at(side, e + CHUNKS)
        return pltpu.make_async_remote_copy(
            ref, ref, ring_send.at[side, e], ring_recv.at[side, e],
            device_id=towards[side], device_id_type=pl.DeviceIdType.MESH)

    def sister_copy(ref, n):
        return pltpu.make_async_remote_copy(
            ref, ref, sis_send.at[n], sis_recv.at[n],
            device_id=sister, device_id_type=pl.DeviceIdType.MESH)

    def lr_at(slot):
        return lrall.at[pl.ds(pl.multiple_of(slot * lr_rows, lr_rows), lr_rows), :]

    def lr_half_at(slot, side):
        rows = lr_rows // 2
        start = pl.multiple_of(slot * lr_rows + side * rows, rows)
        return lrall.at[pl.ds(start, rows), :]

    def lr_ring_copy(ref, side, n):
        return pltpu.make_async_remote_copy(
            ref, ref, lring_send.at[side, n], lring_recv.at[side, n],
            device_id=towards[side], device_id_type=pl.DeviceIdType.MESH)

    def lr_sister_copy(ref, n):
        return pltpu.make_async_remote_copy(
            ref, ref, lsis_send.at[n], lsis_recv.at[n],
            device_id=sister, device_id_type=pl.DeviceIdType.MESH)

    own = gall.at[me]
    own_load = pltpu.make_async_copy(g_hbm, own, load_sem.at[0])
    own_load.start()
    lr_load = pltpu.make_async_copy(lr_hbm, lr_at(me), load_sem.at[1])
    lr_load.start()

    barrier = pltpu.get_barrier_semaphore()
    for peer in (right, left, sister):
        pl.semaphore_signal(barrier, inc=1, device_id=peer, device_id_type=pl.DeviceIdType.MESH)
    pl.semaphore_wait(barrier, 3)

    lr_load.wait()
    for side in (0, 1):
        lr_ring_copy(lr_at(me), side, 0).start()
    own_load.wait()
    for n in range(CHUNKS):
        for side in (0, 1):
            ring_copy(side, n).start()
    lr_sister_copy(lr_at(me), 0).start()
    sister_copy(own, 0).start()

    loads = [pltpu.make_async_copy(l_hbm, lold, load_sem.at[2])]
    rows = r_hbm.shape[0] // LOADS
    for i in range(LOADS):
        part = pl.ds(i * rows, rows)
        loads.append(pltpu.make_async_copy(r_hbm.at[part, :], rnew.at[part, :], load_sem.at[3 + i]))
        loads.append(pltpu.make_async_copy(rr_hbm.at[part, :], rrv.at[part, :], load_sem.at[3 + LOADS + i]))
    for load in loads:
        load.start()

    gt[...] = gall[me].T
    xacc[...] = jnp.zeros_like(xacc)
    lacc[...] = jnp.zeros_like(lacc)
    for load in loads:
        load.wait()

    def event(e):
        dist = e // CHUNKS + 1
        k = e % CHUNKS

        @pl.when(k == 0)
        def _():
            for side in (0, 1):
                slot = 2 * chip_at(side, dist) + core

                @pl.when(dist < half)
                def _():
                    arrived = lr_ring_copy(lr_at(slot), side, dist - 1)
                    arrived.wait_recv()

                    @pl.when(dist < full)
                    def _():
                        lr_ring_copy(lr_at(slot), side, dist).start()

                    @pl.when(dist == full)
                    def _():
                        lr_ring_copy(lr_half_at(slot, side), side, full).start()

                    lr_sister_copy(lr_at(slot), 1 + side * full + dist - 1).start()

                @pl.when(dist == half)
                def _():
                    lr_ring_copy(lr_half_at(slot, side), side, full).wait_recv()
                    lr_sister_copy(lr_half_at(slot, side), 1 + 2 * full + side).start()

        for side in (0, 1):
            ring_arrival(side, e).wait_recv()

            @pl.when(e + CHUNKS < n_events)
            def _():
                ring_copy(side, e + CHUNKS).start()

            slot = 2 * chip_at(side, dist) + core

            @pl.when(dist < half)
            def _():
                @pl.when(k == CHUNKS - 1)
                def _():
                    sister_copy(gall.at[slot], 1 + side * full + dist - 1).start()

            @pl.when(dist == half)
            def _():
                sister_copy(
                    piece_at(side, e + CHUNKS),
                    1 + 2 * full + side * (CHUNKS // 2) + k).start()

    def accumulate(slot):
        cols = pl.ds(pl.multiple_of(slot * block_cols, block_cols), block_cols)
        g = gall[slot]
        rnew[:, cols] = EMA_DECAY * rnew[:, cols] + (1.0 - EMA_DECAY) * _dot(gt[...], g)
        xacc[...] += _dot_nt(g, rrv[:, cols])
        mine = gall[slot, pl.ds(pl.multiple_of(me * lr_rows, lr_rows), lr_rows), :]
        lacc[...] += _dot_nt(mine, g)

    def step(i, _):
        @pl.when(i != n_events - 1)
        def _():
            event(i - i // n_events)

        @pl.when(i < 2)
        def _():
            @pl.when(i == 1)
            def _():
                sister_copy(gall.at[2 * z + (1 - core)], 0).wait_recv()

            accumulate(2 * z + (core + i) % 2)

        @pl.when(i > 2)
        def _():
            q = i - 3
            dist = q // 4 + 1
            side = q % 2
            from_sister = (q % 4) // 2
            src = 2 * ((z + chips + (2 * side - 1) * dist) % chips) + (core + from_sister) % 2

            @pl.when(from_sister == 1)
            def _():
                sister_copy(gall.at[src], 1 + side * full + dist - 1).wait_recv()

            accumulate(src)

        return 0

    lax.fori_loop(0, n_events + 1, step, 0)

    far = chip_at(0, half)
    other = 2 * far + (1 - core)
    for side in (0, 1):
        for k in range(CHUNKS // 2):
            row = (k if side == 0 else k + CHUNKS // 2) * piece
            sister_copy(gall.at[other, pl.ds(row, piece), :],
                        1 + 2 * full + side * (CHUNKS // 2) + k).wait_recv()
        lr_sister_copy(lr_half_at(other, side), 1 + 2 * full + side).wait_recv()
        for dist in range(1, half):
            slot = 2 * chip_at(side, dist) + (1 - core)
            lr_sister_copy(lr_at(slot), 1 + side * full + dist - 1).wait_recv()
    lr_sister_copy(lr_at(2 * z + (1 - core)), 0).wait_recv()

    for side in (0, 1):
        for n in range(n_events):
            ring_copy(side, n).wait_send()
        for dist in range(half):
            slot = 2 * chip_at(side, dist) + core
            ref = lr_at(slot) if dist < full else lr_half_at(slot, side)
            lr_ring_copy(ref, side, dist).wait_send()
        for dist in range(1, half):
            slot = 2 * chip_at(side, dist) + core
            sister_copy(gall.at[slot], 1 + side * full + dist - 1).wait_send()
            lr_sister_copy(lr_at(slot), 1 + side * full + dist - 1).wait_send()
        for k in range(CHUNKS // 2):
            sister_copy(piece_at(side, n_full + CHUNKS + k),
                        1 + 2 * full + side * (CHUNKS // 2) + k).wait_send()
        lr_sister_copy(lr_half_at(2 * far + core, side), 1 + 2 * full + side).wait_send()
    sister_copy(own, 0).wait_send()
    lr_sister_copy(lr_at(me), 0).wait_send()


def _finish_kernel(
    chips,
    gall, lrall, rnew, rrv, xacc, lacc, lold, gt,
    l_out, r_out, d_out,
    rtail, dbuf, lbuf, sem,
):
    me = lax.axis_index("tensor")
    z = me // 2
    far = (z + chips // 2) % chips
    lr_rows = lold.shape[0]
    block_cols = gall.shape[2]
    width = 2 * block_cols

    def chip_cols(chip):
        return pl.ds(pl.multiple_of(chip * width, width), width)

    out = []
    for i in range(1, chips):
        cols = chip_cols((far + i) % chips)
        out.append(pltpu.make_async_copy(rnew.at[:, cols], r_out.at[:, cols], sem.at[i]))
        out[-1].start()

    x = xacc[...]
    left_sum = lacc[...]
    for c in (0, 1):
        slot = 2 * far + c
        cols = pl.ds(pl.multiple_of(slot * block_cols, block_cols), block_cols)
        g = gall[slot]
        x = x + _dot_nt(g, rrv[:, cols])
        mine = gall[slot, pl.ds(pl.multiple_of(me * lr_rows, lr_rows), lr_rows), :]
        left_sum = left_sum + _dot_nt(mine, g)
        rtail[:, c * block_cols:(c + 1) * block_cols] = (
            EMA_DECAY * rnew[:, cols] + (1.0 - EMA_DECAY) * _dot(gt[...], g))
    out.append(pltpu.make_async_copy(rtail, r_out.at[:, chip_cols(far)], sem.at[0]))
    out[-1].start()
    lbuf[...] = EMA_DECAY * lold[...] + (1.0 - EMA_DECAY) * left_sum
    out.append(pltpu.make_async_copy(lbuf, l_out, sem.at[chips]))
    out[-1].start()
    dbuf[...] = _dot(lrall[...], x.astype(jnp.bfloat16))
    out.append(pltpu.make_async_copy(dbuf, d_out, sem.at[chips + 1]))
    out[-1].start()
    for copy in out:
        copy.wait()


def solution(mesh):
    row_spec = P(("layer", "tensor"), None)
    col_spec = P("layer", "tensor")
    chips = mesh.shape["tensor"] // 2
    half = chips // 2
    full = half - 1
    n_events = full * CHUNKS + CHUNKS // 2

    def local_step(g, l, r, lr, rr):
        m, c = g.shape
        n = r.shape[1]
        f32, bf16 = jnp.float32, jnp.bfloat16
        dma = pltpu.SemaphoreType.DMA
        any_spec = pl.BlockSpec(memory_space=pl.ANY)
        vmem_spec = pl.BlockSpec(memory_space=pltpu.VMEM)
        held = (
            pltpu.VMEM((2 * chips, m, c), bf16),
            pltpu.VMEM((m, m), bf16),
            pltpu.VMEM(r.shape, f32),
            pltpu.VMEM(rr.shape, bf16),
            pltpu.VMEM((m, c), f32),
            pltpu.VMEM(l.shape, f32),
            pltpu.VMEM(l.shape, f32),
            pltpu.VMEM((c, m), bf16),
        )
        n_sis = 1 + 2 * full + CHUNKS
        n_lsis = 1 + 2 * full + 2
        state = pl.pallas_call(
            functools.partial(_gather_kernel, chips),
            out_shape=held,
            in_specs=[any_spec] * 5,
            out_specs=[vmem_spec] * len(held),
            scratch_shapes=[
                dma((3 + 2 * LOADS,)),
                dma((2, n_events)), dma((2, n_events)), dma((n_sis,)), dma((n_sis,)),
                dma((2, half)), dma((2, half)), dma((n_lsis,)), dma((n_lsis,)),
            ],
            compiler_params=pltpu.CompilerParams(
                collective_id=0, has_side_effects=True, vmem_limit_bytes=30 * 2**20),
        )(*(pltpu.with_memory_space_constraint(x, pltpu.HBM) for x in (g, lr, l, r, rr)))
        return pl.pallas_call(
            functools.partial(_finish_kernel, chips),
            out_shape=(
                jax.ShapeDtypeStruct(l.shape, f32),
                jax.ShapeDtypeStruct(r.shape, f32),
                jax.ShapeDtypeStruct((m, c), f32),
            ),
            in_specs=[vmem_spec] * len(held),
            out_specs=[any_spec] * 3,
            scratch_shapes=[
                pltpu.VMEM((r.shape[0], 2 * c), f32),
                pltpu.VMEM((m, c), f32),
                pltpu.VMEM(l.shape, f32),
                dma((chips + 2,)),
            ],
            compiler_params=pltpu.CompilerParams(vmem_limit_bytes=30 * 2**20),
        )(*state)

    return jax.shard_map(local_step, mesh=mesh, in_specs=(col_spec, row_spec, row_spec, row_spec, row_spec), out_specs=(row_spec, row_spec, col_spec), check_vma=False)
```
